16 devices in a mesh: dp: 4 (over y, z, core), sp: 4 (over x).
Axes of the slice: x: 4, y: 2, z: 1, core: 2. Of those that a mesh axis runs over, the one named last changes fastest.
The devices are a block of a 4x4x8 slice.
Arguments:
- x: bfloat16 [8192, 2048], P(('dp', 'sp')), parts along dimension 0
- gain: bfloat16 [2048], replicated
- wq: bfloat16 [2048, 2048], replicated
- wk: bfloat16 [2048, 2048], replicated
- wv: bfloat16 [2048, 2048], replicated
- wo: bfloat16 [2048, 2048], replicated
Outputs:
- output: bfloat16 [8192, 2048], P(('dp', 'sp')), parts along dimension 0
There are 4 independent parts. The reference program is written for one: setup_inputs(seed, part) draws one part's arguments, and reference() takes and returns one part's arrays. A program takes and returns all parts, laid end to end along the dimension named above; an argument that names none is the same for every part.
All inputs are finite; a program needn't handle non-finite values.
Results may differ from the reference program's by a relative error of at most 0.012.
Values are sent between devices in bfloat16 or wider.
A program may use at most 768 MiB of HBM per device.

```python
import jax
import jax.numpy as jnp
from jax import lax

ROWS = 2048
D = 2048
HEADS = 16
KV_HEADS = 16
HEAD = 128
THETA = 10000


def setup_inputs(seed: int = 0, part: int = 0) -> dict:
    kx, kn, kq, kk, kv, ko = jax.random.split(jax.random.key(seed), 6)

    def weights(key, rows, columns):
        return jax.random.normal(key, (rows, columns), jnp.float32) * rows**-0.5

    drawn = {
        "x": jax.random.normal(jax.random.fold_in(kx, part), (ROWS, D), jnp.float32),
        "gain": 1 + 0.1 * jax.random.normal(kn, (D,), jnp.float32),
        "wq": 2 * weights(kq, D, HEADS * HEAD),
        "wk": 2 * weights(kk, D, KV_HEADS * HEAD),
        "wv": 4 * weights(kv, D, KV_HEADS * HEAD),
        "wo": weights(ko, HEADS * HEAD, D),
    }
    return {k: v.astype(jnp.bfloat16) for k, v in drawn.items()}


def normed(x, gain):
    wide = x.astype(jnp.float32)
    scale = lax.rsqrt(jnp.mean(wide * wide, -1, keepdims=True) + 1e-6)
    return (wide * scale * gain.astype(jnp.float32)).astype(jnp.bfloat16)


def turned(t, place, theta):
    half = t.shape[-1] // 2
    angle = place.astype(jnp.float32)[:, None] * theta ** (-jnp.arange(half, dtype=jnp.float32) / half)
    cos, sin = jnp.cos(angle)[:, None], jnp.sin(angle)[:, None]
    a, b = t[..., :half].astype(jnp.float32), t[..., half:].astype(jnp.float32)
    return jnp.concatenate([a * cos - b * sin, b * cos + a * sin], -1).astype(jnp.bfloat16)


def matmul(a, w):
    return jnp.dot(a, w, preferred_element_type=jnp.float32).astype(jnp.bfloat16)


def einsum(form, a, b):
    return jnp.einsum(form, a.astype(jnp.float32), b.astype(jnp.float32))


def attention(q, k, v):
    scores = einsum("tgsd,ugd->gstu", q, k) * q.shape[-1] ** -0.5
    token = jnp.arange(q.shape[0])
    scores = jnp.where(token[:, None] >= token, scores, -jnp.inf)
    weights = jax.nn.softmax(scores, -1).astype(jnp.bfloat16)
    return einsum("gstu,ugd->tgsd", weights, v).astype(jnp.bfloat16)


def reference(x, gain, wq, wk, wv, wo):
    a, place = normed(x, gain), jnp.arange(ROWS)
    q = turned(matmul(a, wq).reshape(ROWS, HEADS, HEAD), place, THETA).reshape(ROWS, KV_HEADS, -1, HEAD)
    k = turned(matmul(a, wk).reshape(ROWS, KV_HEADS, HEAD), place, THETA)
    v = matmul(a, wv).reshape(ROWS, KV_HEADS, HEAD)
    seen = attention(q, k, v).reshape(ROWS, HEADS * HEAD)
    return (x.astype(jnp.float32) + jnp.dot(seen, wo, preferred_element_type=jnp.float32)).astype(jnp.bfloat16)
```

```python
import functools

import jax
import jax.numpy as jnp
import numpy as np
from jax import lax
from jax.experimental import pallas as pl
from jax.experimental.pallas import tpu as pltpu
from jax.sharding import PartitionSpec as P

HEAD = 128
THETA = 10000
NEG = -1e30
HIDDEN = 2 * NEG
LOG2E = 1.4426950408889634
MESH = pl.DeviceIdType.MESH
SUB = 128
UNIT = 256
WIDE = 256
SCALE = HEAD**-0.5 * LOG2E


def _dot(a, b):
    return jnp.dot(a, b, preferred_element_type=jnp.float32)


def _turn(t, c, s):
    parts = []
    for i in range(0, t.shape[1], HEAD):
        h = t[:, i : i + HEAD]
        parts.append(h * c + pltpu.roll(h, HEAD // 2, 1) * s)
    return jnp.concatenate(parts, axis=1).astype(jnp.bfloat16)


def _kernel(n, own, x_hbm, gain_ref, wq_hbm, wk_hbm, wv_hbm, wo_hbm, tab_ref, y_hbm, xb, w1_s, wk_s, wv_s, a_s, c_s, s_s, qt_s, acc_s, top_s,
            gap_s, ka_s, va_s, kb_s, vb_s, seen_s, send_sem, recv_sem, load_sem, out_sem):
    me = lax.axis_index("sp")
    right, left = lax.rem(me + 1, n), lax.rem(me + n - 1, n)
    d = x_hbm.shape[1]
    heads = d // HEAD
    groups = d // WIDE
    per = own // SUB
    half = per // 2

    def sub(s):
        return xb.at[pl.ds(s * SUB, SUB), :]

    def send(src, to, s, sem):
        return pltpu.make_async_remote_copy(src_ref=src, dst_ref=sub(s), send_sem=send_sem.at[sem], recv_sem=recv_sem.at[s],
                                            device_id={"sp": to}, device_id_type=MESH)

    def mine(i):
        return x_hbm.at[pl.ds(i * SUB, SUB), :]

    load_x = pltpu.make_async_copy(x_hbm, xb.at[pl.ds(0, own), :], load_sem.at[0])
    load_q = pltpu.make_async_copy(wq_hbm, w1_s, load_sem.at[1])
    load_k = pltpu.make_async_copy(wk_hbm, wk_s, load_sem.at[2])
    load_v = pltpu.make_async_copy(wv_hbm, wv_s, load_sem.at[3])
    load_o = pltpu.make_async_copy(wo_hbm, w1_s, load_sem.at[4])
    load_x.start()
    load_q.start()

    barrier = pltpu.get_barrier_semaphore()
    for to in (left, right):
        pl.semaphore_signal(barrier, inc=1, device_id={"sp": to}, device_id_type=MESH)
    pl.semaphore_wait(barrier, 2)

    @pl.when(me < n - 1)
    def _():
        for i in range(per):
            send(mine(i), right, per + i, i).start()

    @pl.when(me == 0)
    def _():
        for i in range(half):
            send(mine(i), left, 2 * per + i, per + i).start()

    @pl.when(me <= 1)
    def _():
        for i in range(half, per):
            send(mine(i), left, 2 * per + i, per + i).start()

    load_k.start()
    load_v.start()

    def norm(row, at):
        for i in range(0, SUB, 32):
            wide = xb[pl.ds(row + i, 32), :].astype(jnp.float32)
            scale = lax.rsqrt(jnp.mean(wide * wide, -1, keepdims=True) + 1e-6)
            a_s[pl.ds(at + i, 32), :] = (wide * scale * gain_ref[...]).astype(jnp.bfloat16)

    def tables(place, at):
        t = tab_ref[pl.ds(place, SUB), :]
        r = pltpu.roll(t, HEAD // 2, 1)
        low = lax.broadcasted_iota(jnp.int32, t.shape, 1) < HEAD // 2
        c_s[pl.ds(at, SUB), :] = jnp.where(low, t, r)
        s_s[pl.ds(at, SUB), :] = jnp.where(low, -r, t)

    gap_s[...] = lax.broadcasted_iota(jnp.int32, gap_s.shape, 1) - lax.broadcasted_iota(jnp.int32, gap_s.shape, 0)
    top_s[...] = jnp.full(top_s.shape, NEG, jnp.float32)
    load_x.wait()
    for i in range(per):
        norm(i * SUB, i * SUB)
        tables(me * own + i * SUB, i * SUB)
    load_q.wait()

    def q_group(g, _):
        cols = pl.ds(pl.multiple_of(g * WIDE, WIDE), WIDE)
        q = _dot(a_s[...], w1_s[:, cols]).astype(jnp.bfloat16).astype(jnp.float32)
        qt_s[cols, :] = _turn(q, c_s[...], s_s[...]).T
        return None

    lax.fori_loop(0, groups, q_group, None)
    load_o.start()
    load_k.wait()
    load_v.wait()

    def unit(u, _):
        t = u - 2
        last = me == n - 1
        s0 = jnp.where(u < 2, 2 * u, jnp.where(last, jnp.where(t < per, per + t, 2 * per + t), jnp.where(t < half, per + 2 * t, 2 * per + 2 * t)))
        s1 = jnp.where(u < 2, 2 * u + 1,
                       jnp.where(last, jnp.where(t < per, 2 * per + t, 2 * per + half + t), jnp.where(t < half, per + 2 * t + 1, 2 * per + 2 * t + 1)))

        def place(s):
            slot = s // per
            chunk = jnp.where(slot == 0, me, jnp.where(slot == 1, left, jnp.where(slot == 2, right, lax.rem(me + 2, n))))
            return chunk * own + lax.rem(s, per) * SUB

        at = pl.multiple_of(lax.rem(u, 2) * UNIT, UNIT)
        level = jnp.where(u < 2, u * UNIT, -(2**20))

        @pl.when(u >= 2)
        def _():
            for s in (s0, s1):
                send(sub(s), right, s, 0).wait_recv()

            @pl.when((t == 0) & (me < n - 1))
            def _():
                for i in range(half):
                    send(sub(per + i), right, 3 * per + i, 2 * per + i).start()

            @pl.when(last & (t >= half) & (t < per))
            def _():
                send(sub(2 * per + t), left, 3 * per + t, 2 * per + t - half).start()

            for i, s in enumerate((s0, s1)):
                norm(pl.multiple_of(s * SUB, SUB), at + i * SUB)
                tables(pl.multiple_of(place(s), SUB), at + i * SUB)

        def project(g, k_ref, v_ref):
            cols = pl.ds(pl.multiple_of(g * WIDE, WIDE), WIDE)
            rows = pl.ds(at, UNIT)
            a = a_s[rows, :]
            k = _dot(a, wk_s[:, cols]).astype(jnp.bfloat16).astype(jnp.float32)
            k_ref[...] = _turn(k, c_s[rows, :], s_s[rows, :])
            v = _dot(a, wv_s[:, cols]).astype(jnp.bfloat16)
            v_ref[...] = v.T

        ones = jnp.ones((8, UNIT), jnp.bfloat16)

        def attend(g, k_ref, v_ref):
            ok = gap_s[...] >= level
            for i in range(WIDE // HEAD):
                h = g * (WIDE // HEAD) + i
                k = k_ref[:, i * HEAD : (i + 1) * HEAD]
                q = qt_s[pl.ds(pl.multiple_of(h * HEAD, HEAD), HEAD), :]
                s = jnp.where(ok, _dot(k, q), HIDDEN)
                old = top_s[h]
                top = jnp.maximum(old, s.max(axis=0, keepdims=True))
                top_s[h] = top
                p = jnp.exp2((s - top) * SCALE).astype(jnp.bfloat16)
                keep = jnp.exp2((old - top) * SCALE)
                values = jnp.concatenate([v_ref[i * HEAD : (i + 1) * HEAD, :], ones], axis=0)
                acc_s[h] = acc_s[h] * keep + _dot(values, p)

        project(0, ka_s, va_s)

        def pair(j, _):
            project(2 * j + 1, kb_s, vb_s)
            attend(2 * j, ka_s, va_s)
            project(2 * j + 2, ka_s, va_s)
            attend(2 * j + 1, kb_s, vb_s)
            return None

        lax.fori_loop(0, groups // 2 - 1, pair, None)
        project(groups - 1, kb_s, vb_s)
        attend(groups - 2, ka_s, va_s)
        attend(groups - 1, kb_s, vb_s)
        return None

    acc_s[...] = jnp.zeros(acc_s.shape, jnp.float32)
    lax.fori_loop(0, 2, unit, None)

    @pl.when(me == 0)
    def _():
        for i in range(half):
            send(sub(2 * per + half + i), left, 2 * per + half + i, 0).wait_recv()
            send(sub(2 * per + half + i), left, 3 * per + half + i, 2 * per + i).start()

    lax.fori_loop(2, 2 + 2 * me, unit, None)

    def finish(h, _):
        o = acc_s[h, :HEAD, :] * (1 / acc_s[h, HEAD : HEAD + 1, :])
        seen_s[:, pl.ds(pl.multiple_of(h * HEAD, HEAD), HEAD)] = o.T.astype(jnp.bfloat16)
        return None

    lax.fori_loop(0, heads, finish, None)
    load_o.wait()

    def out(g):
        cols = pl.ds(pl.multiple_of(g * WIDE, WIDE), WIDE)
        return pltpu.make_async_copy(a_s.at[:, cols], y_hbm.at[:, cols], out_sem.at[g])

    def y_group(g, _):
        cols = pl.ds(pl.multiple_of(g * WIDE, WIDE), WIDE)
        y = _dot(seen_s[...], w1_s[:, cols])
        a_s[:, cols] = (xb[pl.ds(0, own), cols].astype(jnp.float32) + y).astype(jnp.bfloat16)
        out(g).start()
        return None

    lax.fori_loop(0, groups, y_group, None)
    for g in range(groups):
        out(g).wait()

    @pl.when(me < n - 1)
    def _():
        for i in range(per):
            send(mine(i), right, per + i, i).wait_send()

    @pl.when(me == 0)
    def _():
        for i in range(half):
            send(mine(i), left, 2 * per + i, per + i).wait_send()

    @pl.when(me <= 1)
    def _():
        for i in range(half, per):
            send(mine(i), left, 2 * per + i, per + i).wait_send()

    for i in range(half):
        send(sub(per + i), right, 3 * per + i, 2 * per + i).wait_send()


def _table(tokens):
    half = HEAD // 2
    angle = np.arange(tokens, dtype=np.float32)[:, None] * np.power(np.float32(THETA), -np.arange(half, dtype=np.float32) / np.float32(half))
    angle = angle.astype(np.float32)
    return np.concatenate([np.cos(angle), np.sin(angle)], axis=1).astype(np.float32)


def solution(mesh):
    n = mesh.shape["sp"]

    def step(x, gain, wq, wk, wv, wo):
        own, d = x.shape
        heads = d // HEAD
        bf16, f32 = jnp.bfloat16, jnp.float32
        anywhere, vmem = pl.BlockSpec(memory_space=pl.ANY), pl.BlockSpec(memory_space=pltpu.VMEM)
        tokens = n * own
        return pl.pallas_call(
            functools.partial(_kernel, n, own),
            out_shape=jax.ShapeDtypeStruct((own, d), bf16),
            in_specs=[anywhere, vmem, anywhere, anywhere, anywhere, anywhere, vmem],
            out_specs=anywhere,
            scratch_shapes=[
                pltpu.VMEM((n * own, d), bf16),
                pltpu.VMEM((d, d), bf16),
                pltpu.VMEM((d, d), bf16),
                pltpu.VMEM((d, d), bf16),
                pltpu.VMEM((own, d), bf16),
                pltpu.VMEM((own, HEAD), f32),
                pltpu.VMEM((own, HEAD), f32),
                pltpu.VMEM((d, own), bf16),
                pltpu.VMEM((heads, HEAD + 8, own), f32),
                pltpu.VMEM((heads, 1, own), f32),
                pltpu.VMEM((UNIT, own), jnp.int32),
                pltpu.VMEM((UNIT, WIDE), bf16),
                pltpu.VMEM((WIDE, UNIT), bf16),
                pltpu.VMEM((UNIT, WIDE), bf16),
                pltpu.VMEM((WIDE, UNIT), bf16),
                pltpu.VMEM((own, d), bf16),
                pltpu.SemaphoreType.DMA((3 * (own // SUB),)),
                pltpu.SemaphoreType.DMA((4 * (own // SUB),)),
                pltpu.SemaphoreType.DMA((5,)),
                pltpu.SemaphoreType.DMA((d // WIDE,)),
            ],
            compiler_params=pltpu.CompilerParams(collective_id=0, has_side_effects=True, vmem_limit_bytes=60 * 2**20),
        )(x, gain.astype(f32)[None], wq, wk, wv, wo, jnp.asarray(_table(tokens)))

    tokens, whole = P(("dp", "sp"), None), P(None, None)
    return jax.shard_map(
        step,
        mesh=mesh,
        in_specs=(tokens, P(None), whole, whole, whole, whole),
        out_specs=tokens,
        check_vma=False,
    )
```

```python
import functools

import jax
import jax.numpy as jnp
import numpy as np
from jax import lax
from jax.experimental import pallas as pl
from jax.experimental.pallas import tpu as pltpu
from jax.sharding import PartitionSpec as P

HEAD = 128
THETA = 10000
NEG = -1e30
HIDDEN = 2 * NEG
LOG2E = 1.4426950408889634
MESH = pl.DeviceIdType.MESH
VMEM = 54 * 2**20
SUB = 64
UNIT = 256
WIDE = 512
SCALE = HEAD**-0.5 * LOG2E


def _dot(a, b):
    return jnp.dot(a, b, preferred_element_type=jnp.float32)


def _turn(t, c, s):
    parts = []
    for i in range(0, t.shape[1], HEAD):
        h = t[:, i : i + HEAD]
        parts.append(h * c + pltpu.roll(h, HEAD // 2, 1) * s)
    return jnp.concatenate(parts, axis=1).astype(jnp.bfloat16)


def _kernel(n, own, x_hbm, gain_ref, wq_hbm, wk_hbm, wv_hbm, wo_hbm, tab_ref, y_hbm, xb, w1_s, wk_s, wv_s, own_s, n_s, nc_s, ns_s, oc_s, os_s, qt_s,
            acc_s, top_s, gap_s, ka_s, va_s, kb_s, vb_s, y_s, send_sem, recv_sem, load_sem, out_sem):
    me = lax.axis_index("sp")
    right, left = lax.rem(me + 1, n), lax.rem(me + n - 1, n)
    last = me == n - 1
    d = x_hbm.shape[1]
    groups = d // WIDE
    each = WIDE // HEAD
    per = own // SUB
    half = per // 2
    k_refs, v_refs = (ka_s, kb_s), (va_s, vb_s)

    def sub(s):
        return xb.at[pl.ds(pl.multiple_of(s * SUB, SUB), SUB), :]

    def send(src, to, s, sem):
        return pltpu.make_async_remote_copy(src_ref=src, dst_ref=sub(s), send_sem=send_sem.at[sem], recv_sem=recv_sem.at[s],
                                            device_id={"sp": to}, device_id_type=MESH)

    def mine(i):
        return x_hbm.at[pl.ds(i * SUB, SUB), :]

    def arrived(s, count):
        for i in range(count):
            send(sub(s + i), right, s + i, 0).wait_recv()

    def pass_on(s, count, to, target, sem):
        for i in range(count):
            send(sub(s + i), to, target + i, sem + i).start()

    def passed(count, sem):
        for i in range(count):
            send(sub(per + i), right, 3 * per + i, sem + i).wait_send()

    def columns(g):
        return pl.ds(pl.multiple_of(g * WIDE, WIDE), WIDE)

    def load_q(g):
        return pltpu.make_async_copy(wq_hbm.at[:, columns(g)], w1_s.at[:, columns(g)], load_sem.at[4 + g])

    load_x = pltpu.make_async_copy(x_hbm, xb.at[pl.ds(0, own), :], load_sem.at[0])
    load_k = pltpu.make_async_copy(wk_hbm, wk_s, load_sem.at[1])
    load_v = pltpu.make_async_copy(wv_hbm, wv_s, load_sem.at[2])
    load_o = pltpu.make_async_copy(wo_hbm, w1_s, load_sem.at[3])
    load_x.start()
    for g in range(groups):
        load_q(g).start()

    barrier = pltpu.get_barrier_semaphore()
    for to in (left, right):
        pl.semaphore_signal(barrier, inc=1, device_id={"sp": to}, device_id_type=MESH)
    pl.semaphore_wait(barrier, 2)

    @pl.when(me < n - 1)
    def _():
        for i in range(per):
            send(mine(i), right, per + i, i).start()

    @pl.when(me == 0)
    def _():
        for i in range(half):
            send(mine(i), left, 2 * per + i, per + i).start()

    @pl.when(me <= 1)
    def _():
        for i in range(half, per):
            send(mine(i), left, 2 * per + i, per + i).start()

    load_k.start()
    load_v.start()

    def norm(row, ref, at, rows):
        gain = gain_ref[...].astype(jnp.float32)
        for i in range(0, rows, 16):
            wide = xb[pl.ds(row + i, 16), :].astype(jnp.float32)
            scale = lax.rsqrt(jnp.mean(wide * wide, -1, keepdims=True) + 1e-6)
            ref[at + i : at + i + 16, :] = (wide * scale * gain).astype(jnp.bfloat16)

    def tables(place, c_ref, s_ref, at, rows):
        t = tab_ref[pl.ds(place, rows), :]
        r = pltpu.roll(t, HEAD // 2, 1)
        low = lax.broadcasted_iota(jnp.int32, t.shape, 1) < HEAD // 2
        c_ref[at : at + rows, :] = jnp.where(low, t, r)
        s_ref[at : at + rows, :] = jnp.where(low, -r, t)

    gap_s[...] = lax.broadcasted_iota(jnp.int32, gap_s.shape, 1) - lax.broadcasted_iota(jnp.int32, gap_s.shape, 0)
    top_s[...] = jnp.full(top_s.shape, NEG, jnp.float32)
    acc_s[...] = jnp.zeros(acc_s.shape, jnp.float32)
    load_x.wait()
    norm(0, own_s, 0, own)
    tables(pl.multiple_of(me * own, own), oc_s, os_s, 0, own)

    def q_group(g, _):
        load_q(g).wait()
        q = _dot(own_s[...], w1_s[:, columns(g)]).astype(jnp.bfloat16).astype(jnp.float32)
        qt_s[columns(g), :] = _turn(q, oc_s[...], os_s[...]).T
        return None

    lax.fori_loop(0, groups, q_group, None)
    load_o.start()
    load_k.wait()
    load_v.wait()

    def unit(rows, least, a_ref, c_ref, s_ref, at):
        ones = jnp.ones((8, rows), jnp.bfloat16)
        span = pl.ds(at, rows)

        def score(g, i):
            h = g * each + i
            s = _dot(k_refs[g % 2][:rows, i * HEAD : (i + 1) * HEAD], qt_s[h * HEAD : (h + 1) * HEAD, :])
            return s if least is None else jnp.where(gap_s[:rows, :] >= least, s, HIDDEN)

        def weigh(h, s):
            old = top_s[h]
            top = jnp.maximum(old, s.max(axis=0, keepdims=True))
            top_s[h] = top
            return jnp.exp2((s - top) * SCALE).astype(jnp.bfloat16), jnp.exp2((old - top) * SCALE)

        def mix(g, i, p, keep):
            h = g * each + i
            values = jnp.concatenate([v_refs[g % 2][i * HEAD : (i + 1) * HEAD, :rows], ones], axis=0)
            acc_s[h] = acc_s[h] * keep + _dot(values, p)

        def step(ga, gp):
            if ga is not None:
                s = [score(ga, i) for i in range(each)]
            if gp is not None:
                k = _dot(a_ref[span, :], wk_s[:, columns(gp)])
            if ga is not None:
                w = [weigh(ga * each + i, s[i]) for i in range(each)]
            if gp is not None:
                v = _dot(a_ref[span, :], wv_s[:, columns(gp)])
                k_refs[gp % 2][:rows, :] = _turn(k.astype(jnp.bfloat16).astype(jnp.float32), c_ref[span, :], s_ref[span, :])
            if ga is not None:
                for i in range(each):
                    mix(ga, i, *w[i])
            if gp is not None:
                v_refs[gp % 2][:, :rows] = v.astype(jnp.bfloat16).T

        step(None, 0)
        for g in range(1, groups):
            step(g - 1, g)
        step(groups - 1, None)

    pair = UNIT // SUB // 2

    def from_first(i):
        arrived(2 * per + pair * i, pair)
        pass_on(2 * per + pair * i, pair, left, 3 * per + pair * i, 2 * per + pair * i)

    def own_unit(u, _):
        @pl.when(last & (u == 1))
        def _():
            from_first(0)

        at = pl.multiple_of(u * UNIT, UNIT)
        unit(UNIT, at, own_s, oc_s, os_s, at)
        return None

    lax.fori_loop(0, own // UNIT, own_unit, None)

    @pl.when(me == 0)
    def _():
        arrived(2 * per + half, half)
        pass_on(2 * per + half, half, left, 3 * per + half, 2 * per)

    def place(s):
        slot = s // per
        chunk = jnp.where(slot == 0, me, jnp.where(slot == 1, left, jnp.where(slot == 2, right, lax.rem(me + 2, n))))
        return pl.multiple_of(chunk * own + lax.rem(s, per) * SUB, SUB)

    def received(s0, s1, count):
        rows = 2 * count * SUB
        for i, s in enumerate((s0, s1)):
            norm(pl.multiple_of(s * SUB, SUB), n_s, i * count * SUB, count * SUB)
            tables(place(s), nc_s, ns_s, i * count * SUB, count * SUB)
        unit(rows, None, n_s, nc_s, ns_s, 0)

    def large(t, _):
        s0 = jnp.where(last, per + pair * t, jnp.where((me < n - 2) | (lax.rem(t, 2) == 0), per + jnp.where(me < n - 2, 2, 1) * pair * t, 3 * per + pair * (t - 1)))
        s1 = jnp.where(last, 2 * per + pair * t, s0 + pair)
        arrived(s0, pair)

        @pl.when(me < n - 1)
        def _():
            arrived(s1, pair)

        @pl.when((me == n - 2) & (t == 0))
        def _():
            pass_on(per, half, right, 3 * per, 2 * per)

        @pl.when(last & (t != 1))
        def _():
            from_first(jnp.maximum(t, 1))

        received(s0, s1, pair)
        return None

    lax.fori_loop(0, jnp.where(last, per // pair, me * (own // UNIT)), large, None)

    def small(t, _):
        s0, s1 = 3 * per + t, 3 * per + half + t
        arrived(s0, 1)
        arrived(s1, 1)
        received(s0, s1, 1)
        return None

    lax.fori_loop(0, jnp.where(last, half, 0), small, None)

    for h in range(d // HEAD):
        o = acc_s[h, :HEAD, :] * (1 / acc_s[h, HEAD : HEAD + 1, :])
        own_s[:, h * HEAD : (h + 1) * HEAD] = o.T.astype(jnp.bfloat16)
    load_o.wait()

    def out(g):
        return pltpu.make_async_copy(y_s.at[:, columns(g)], y_hbm.at[:, columns(g)], out_sem.at[g])

    for g in range(groups):
        y = _dot(own_s[...], w1_s[:, columns(g)])
        y_s[:, columns(g)] = (xb[0:own, columns(g)].astype(jnp.float32) + y).astype(jnp.bfloat16)
        out(g).start()

    @pl.when(me < n - 1)
    def _():
        for i in range(per):
            send(mine(i), right, per + i, i).wait_send()

    @pl.when(me == 0)
    def _():
        for i in range(half):
            send(mine(i), left, 2 * per + i, per + i).wait_send()

    @pl.when(me <= 1)
    def _():
        for i in range(half, per):
            send(mine(i), left, 2 * per + i, per + i).wait_send()

    @pl.when((me == 0) | (me == n - 2))
    def _():
        passed(half, 2 * per)

    @pl.when(last)
    def _():
        passed(per, 2 * per)

    for g in range(groups):
        out(g).wait()


def _table(tokens):
    half = HEAD // 2
    angle = np.arange(tokens, dtype=np.float32)[:, None] * np.power(np.float32(THETA), -np.arange(half, dtype=np.float32) / np.float32(half))
    angle = angle.astype(np.float32)
    return np.concatenate([np.cos(angle), np.sin(angle)], axis=1).astype(np.float32)


def solution(mesh):
    n = mesh.shape["sp"]

    def step(x, gain, wq, wk, wv, wo):
        own, d = x.shape
        heads = d // HEAD
        bf16, f32 = jnp.bfloat16, jnp.float32
        anywhere, vmem = pl.BlockSpec(memory_space=pl.ANY), pl.BlockSpec(memory_space=pltpu.VMEM)
        tokens = n * own
        return pl.pallas_call(
            functools.partial(_kernel, n, own),
            out_shape=jax.ShapeDtypeStruct((own, d), bf16),
            in_specs=[anywhere, vmem, anywhere, anywhere, anywhere, anywhere, vmem],
            out_specs=anywhere,
            scratch_shapes=[
                pltpu.VMEM((n * own, d), bf16),
                pltpu.VMEM((d, d), bf16),
                pltpu.VMEM((d, d), bf16),
                pltpu.VMEM((d, d), bf16),
                pltpu.VMEM((own, d), bf16),
                pltpu.VMEM((UNIT, d), bf16),
                *[pltpu.VMEM((UNIT, HEAD), f32)] * 2,
                *[pltpu.VMEM((own, HEAD), f32)] * 2,
                pltpu.VMEM((d, own), bf16),
                pltpu.VMEM((heads, HEAD + 8, own), f32),
                pltpu.VMEM((heads, 1, own), f32),
                pltpu.VMEM((UNIT, own), jnp.int32),
                pltpu.VMEM((UNIT, WIDE), bf16),
                pltpu.VMEM((WIDE, UNIT), bf16),
                pltpu.VMEM((UNIT, WIDE), bf16),
                pltpu.VMEM((WIDE, UNIT), bf16),
                pltpu.VMEM((own, d), bf16),
                pltpu.SemaphoreType.DMA((3 * (own // SUB),)),
                pltpu.SemaphoreType.DMA((4 * (own // SUB),)),
                pltpu.SemaphoreType.DMA((4 + d // WIDE,)),
                pltpu.SemaphoreType.DMA((d // WIDE,)),
            ],
            compiler_params=pltpu.CompilerParams(collective_id=0, has_side_effects=True, vmem_limit_bytes=VMEM),
        )(x, gain[None], wq, wk, wv, wo, jnp.asarray(_table(tokens)))

    tokens, whole = P(("dp", "sp"), None), P(None, None)
    return jax.shard_map(
        step,
        mesh=mesh,
        in_specs=(tokens, P(None), whole, whole, whole, whole),
        out_specs=tokens,
        check_vma=False,
    )
```

```python
import functools

import jax
import jax.numpy as jnp
import numpy as np
from jax import lax
from jax.experimental import pallas as pl
from jax.experimental.pallas import tpu as pltpu
from jax.sharding import PartitionSpec as P

HEAD = 128
THETA = 10000
NEG = -1e30
HIDDEN = 2 * NEG
LOG2E = 1.4426950408889634
MESH = pl.DeviceIdType.MESH
VMEM = 54 * 2**20
SUB = 64
UNIT = 256
WIDE = 512
SCALE = HEAD**-0.5 * LOG2E


def _dot(a, b):
    return jnp.dot(a, b, preferred_element_type=jnp.float32)


def _turn(t, c, s):
    parts = []
    for i in range(0, t.shape[1], HEAD):
        h = t[:, i : i + HEAD]
        parts.append(h * c + pltpu.roll(h, HEAD // 2, 1) * s)
    return jnp.concatenate(parts, axis=1).astype(jnp.bfloat16)


def _kernel(n, own, x_hbm, gain_ref, wq_hbm, wk_hbm, wv_hbm, wo_hbm, tab_hbm, y_ref, x_s, ab, w1_s, wk_s, wv_s, seen_s, tab_s, nc_s, ns_s, oc_s, os_s,
            qt_s, acc_s, top_s, gap_s, ka_s, va_s, kb_s, vb_s, send_sem, recv_sem, load_sem):
    me = lax.axis_index("sp")
    right, left = lax.rem(me + 1, n), lax.rem(me + n - 1, n)
    last = me == n - 1
    d = x_hbm.shape[1]
    groups = d // WIDE
    each = WIDE // HEAD
    per = own // SUB
    half = per // 2
    pair = UNIT // SUB // 2
    k_refs, v_refs = (ka_s, kb_s), (va_s, vb_s)

    def sub(s):
        return ab.at[pl.ds(pl.multiple_of(s * SUB, SUB), SUB), :]

    def send(src, to, s, sem):
        return pltpu.make_async_remote_copy(src_ref=src, dst_ref=sub(s), send_sem=send_sem.at[sem], recv_sem=recv_sem.at[s],
                                            device_id={"sp": to}, device_id_type=MESH)

    def arrived(s, count):
        for i in range(count):
            send(sub(s + i), right, s + i, 0).wait_recv()

    def pass_on(s, count, to, target, sem):
        for i in range(count):
            send(sub(s + i), to, target + i, sem + i).start()

    def passed(count, sem):
        for i in range(count):
            send(sub(per + i), right, 3 * per + i, sem + i).wait_send()

    def columns(g):
        return pl.ds(pl.multiple_of(g * WIDE, WIDE), WIDE)

    def load_x(i):
        return pltpu.make_async_copy(x_hbm.at[pl.ds(i * SUB, SUB), :], x_s.at[pl.ds(i * SUB, SUB), :], load_sem.at[4 + groups + i])

    def load_q(g):
        return pltpu.make_async_copy(wq_hbm.at[:, columns(g)], w1_s.at[:, columns(g)], load_sem.at[4 + g])

    load_t = pltpu.make_async_copy(tab_hbm, tab_s, load_sem.at[0])
    load_k = pltpu.make_async_copy(wk_hbm, wk_s, load_sem.at[1])
    load_v = pltpu.make_async_copy(wv_hbm, wv_s, load_sem.at[2])
    load_o = pltpu.make_async_copy(wo_hbm, w1_s, load_sem.at[3])
    for i in range(per):
        load_x(i).start()
    load_t.start()
    for g in range(groups):
        load_q(g).start()
    load_k.start()
    load_v.start()

    barrier = pltpu.get_barrier_semaphore()
    for to in (left, right):
        pl.semaphore_signal(barrier, inc=1, device_id={"sp": to}, device_id_type=MESH)

    def norm(i):
        load_x(i).wait()
        gain = gain_ref[...].astype(jnp.float32)[None]
        for r in range(i * SUB, (i + 1) * SUB, 16):
            wide = x_s[r : r + 16, :].astype(jnp.float32)
            scale = lax.rsqrt(jnp.mean(wide * wide, -1, keepdims=True) + 1e-6)
            ab[r : r + 16, :] = (wide * scale * gain).astype(jnp.bfloat16)

    def tables(s, c_ref, s_ref, at, count):
        slot = s // per
        chunk = jnp.where(slot == 0, me, jnp.where(slot == 1, left, jnp.where(slot == 2, right, lax.rem(me + 2, n))))
        first = chunk * per + lax.rem(s, per)
        c, z = tab_s[0:SUB, :], tab_s[SUB : 2 * SUB, :]
        for i in range(count):
            base = [tab_s[pl.ds(2 * SUB + k * n * per + first + i, 1), :] for k in range(4)]
            c_ref[at + i * SUB : at + (i + 1) * SUB, :] = base[0] * c - base[1] * z
            s_ref[at + i * SUB : at + (i + 1) * SUB, :] = base[2] * c + base[3] * z

    def send_own(i):
        @pl.when(me < n - 1)
        def _():
            send(sub(i), right, per + i, i).start()

        @pl.when((me == 0) if i < half else (me <= 1))
        def _():
            send(sub(i), left, 2 * per + i, per + i).start()

    norm(0)
    norm(1)
    pl.semaphore_wait(barrier, 2)
    for i in range(per):
        send_own(i)
        if i + 2 < per:
            norm(i + 2)

    gap_s[...] = lax.broadcasted_iota(jnp.int32, gap_s.shape, 1) - lax.broadcasted_iota(jnp.int32, gap_s.shape, 0)
    top_s[...] = jnp.full(top_s.shape, NEG, jnp.float32)
    acc_s[...] = jnp.zeros(acc_s.shape, jnp.float32)
    load_t.wait()
    tables(0, oc_s, os_s, 0, per)

    def q_group(g, _):
        load_q(g).wait()
        q = _dot(ab[0:own, :], w1_s[:, columns(g)]).astype(jnp.bfloat16).astype(jnp.float32)
        qt_s[columns(g), :] = _turn(q, oc_s[...], os_s[...]).T
        return None

    lax.fori_loop(0, groups, q_group, None)
    load_o.start()
    load_k.wait()
    load_v.wait()

    def finish(h):
        o = acc_s[h, :HEAD, :] * (1 / acc_s[h, HEAD : HEAD + 1, :])
        seen_s[:, h * HEAD : (h + 1) * HEAD] = o.T.astype(jnp.bfloat16)

    def unit(s0, s1, count, c_ref, s_ref, at, least=None, final=False):
        rows = 2 * count * SUB
        ones = jnp.ones((8, rows), jnp.bfloat16)
        span = pl.ds(at, rows)

        def states():
            return jnp.concatenate([ab[pl.ds(pl.multiple_of(s * SUB, SUB), count * SUB), :] for s in (s0, s1)], axis=0)

        def score(g, i):
            h = g * each + i
            s = _dot(k_refs[g % 2][:rows, i * HEAD : (i + 1) * HEAD], qt_s[h * HEAD : (h + 1) * HEAD, :])
            return s if least is None else jnp.where(gap_s[:rows, :] >= least, s, HIDDEN)

        def weigh(h, s):
            old = top_s[h]
            top = jnp.maximum(old, s.max(axis=0, keepdims=True))
            top_s[h] = top
            return jnp.exp2((s - top) * SCALE).astype(jnp.bfloat16), jnp.exp2((old - top) * SCALE)

        def mix(g, i, p, keep):
            h = g * each + i
            values = jnp.concatenate([v_refs[g % 2][i * HEAD : (i + 1) * HEAD, :rows], ones], axis=0)
            acc_s[h] = acc_s[h] * keep + _dot(values, p)

        def step(ga, gp):
            if ga is not None:
                s = [score(ga, i) for i in range(each)]
            if gp is not None:
                k = _dot(states(), wk_s[:, columns(gp)])
            if ga is not None:
                w = [weigh(ga * each + i, s[i]) for i in range(each)]
            if gp is not None:
                v = _dot(states(), wv_s[:, columns(gp)])
                k_refs[gp % 2][:rows, :] = _turn(k.astype(jnp.bfloat16).astype(jnp.float32), c_ref[span, :], s_ref[span, :])
            if ga is not None:
                for i in range(each):
                    mix(ga, i, *w[i])
            if gp is not None:
                v_refs[gp % 2][:, :rows] = v.astype(jnp.bfloat16).T
            if final and ga is not None:
                for i in range(each):
                    finish(ga * each + i)

        step(None, 0)
        for g in range(1, groups):
            step(g - 1, g)
        step(groups - 1, None)

    def from_first(i):
        arrived(2 * per + pair * i, pair)
        pass_on(2 * per + pair * i, pair, left, 3 * per + pair * i, 2 * per + pair * i)

    def own_unit(u, _):
        @pl.when(last & (u == 1))
        def _():
            from_first(0)

        at = pl.multiple_of(u * UNIT, UNIT)
        unit(2 * pair * u, 2 * pair * u + pair, pair, oc_s, os_s, at, least=at)
        return None

    lax.fori_loop(0, own // UNIT, own_unit, None)

    @pl.when(me == 0)
    def _():
        arrived(2 * per + half, half)
        pass_on(2 * per + half, half, left, 3 * per + half, 2 * per)

    def received(s0, s1, count, final=False):
        for i, s in enumerate((s0, s1)):
            tables(s, nc_s, ns_s, i * count * SUB, count)
        unit(s0, s1, count, nc_s, ns_s, 0, final=final)

    def large(t, _):
        s0 = jnp.where(last, per + pair * t, jnp.where((me < n - 2) | (lax.rem(t, 2) == 0), per + jnp.where(me < n - 2, 2, 1) * pair * t, 3 * per + pair * (t - 1)))
        s1 = jnp.where(last, 2 * per + pair * t, s0 + pair)
        arrived(s0, pair)

        @pl.when(me < n - 1)
        def _():
            arrived(s1, pair)

        @pl.when((me == n - 2) & (t == 0))
        def _():
            pass_on(per, half, right, 3 * per, 2 * per)

        @pl.when(last & (t != 1))
        def _():
            from_first(jnp.maximum(t, 1))

        received(s0, s1, pair)
        return None

    lax.fori_loop(0, jnp.where(last, per // pair, me * (own // UNIT)), large, None)

    def small(t, _):
        s0, s1 = 3 * per + t, 3 * per + half + t
        arrived(s0, 1)
        arrived(s1, 1)
        received(s0, s1, 1)
        return None

    @pl.when(last)
    def _():
        lax.fori_loop(0, half - 1, small, None)
        s0, s1 = 3 * per + half - 1, 3 * per + per - 1
        arrived(s0, 1)
        arrived(s1, 1)
        received(s0, s1, 1, final=True)

    @pl.when(me < n - 1)
    def _():
        for h in range(d // HEAD):
            finish(h)

    load_o.wait()
    for g in range(groups):
        y = _dot(seen_s[...], w1_s[:, columns(g)])
        y_ref[:, columns(g)] = (x_s[:, columns(g)].astype(jnp.float32) + y).astype(jnp.bfloat16)

    for i in range(per):
        @pl.when(me < n - 1)
        def _():
            send(sub(i), right, per + i, i).wait_send()

        @pl.when((me == 0) if i < half else (me <= 1))
        def _():
            send(sub(i), left, 2 * per + i, per + i).wait_send()

    @pl.when((me == 0) | (me == n - 2))
    def _():
        passed(half, 2 * per)

    @pl.when(last)
    def _():
        passed(per, 2 * per)


def _table(tokens):
    half = HEAD // 2
    rate = np.tile(np.power(float(THETA), -np.arange(half) / half), 2)
    sign = np.repeat([-1.0, 1.0], half)
    inner, outer = (np.asarray(p)[:, None] * rate for p in (np.arange(SUB), np.arange(0, tokens, SUB)))
    return np.concatenate([np.cos(inner), np.sin(inner), np.cos(outer), np.sin(outer), sign * np.sin(outer), sign * np.cos(outer)]).astype(np.float32)


def solution(mesh):
    n = mesh.shape["sp"]

    def step(x, gain, wq, wk, wv, wo):
        own, d = x.shape
        heads = d // HEAD
        bf16, f32 = jnp.bfloat16, jnp.float32
        anywhere, vmem = pl.BlockSpec(memory_space=pl.ANY), pl.BlockSpec(memory_space=pltpu.VMEM)
        table = _table(n * own)
        return pl.pallas_call(
            functools.partial(_kernel, n, own),
            out_shape=pltpu.VMEM((own, d), bf16),
            in_specs=[anywhere, vmem, anywhere, anywhere, anywhere, anywhere, anywhere],
            out_specs=vmem,
            scratch_shapes=[
                pltpu.VMEM((own, d), bf16),
                pltpu.VMEM((n * own, d), bf16),
                pltpu.VMEM((d, d), bf16),
                pltpu.VMEM((d, d), bf16),
                pltpu.VMEM((d, d), bf16),
                pltpu.VMEM((own, d), bf16),
                pltpu.VMEM(table.shape, f32),
                *[pltpu.VMEM((UNIT, HEAD), f32)] * 2,
                *[pltpu.VMEM((own, HEAD), f32)] * 2,
                pltpu.VMEM((d, own), bf16),
                pltpu.VMEM((heads, HEAD + 8, own), f32),
                pltpu.VMEM((heads, 1, own), f32),
                pltpu.VMEM((UNIT, own), jnp.int32),
                pltpu.VMEM((UNIT, WIDE), bf16),
                pltpu.VMEM((WIDE, UNIT), bf16),
                pltpu.VMEM((UNIT, WIDE), bf16),
                pltpu.VMEM((WIDE, UNIT), bf16),
                pltpu.SemaphoreType.DMA((3 * (own // SUB),)),
                pltpu.SemaphoreType.DMA((4 * (own // SUB),)),
                pltpu.SemaphoreType.DMA((4 + d // WIDE + own // SUB,)),
            ],
            compiler_params=pltpu.CompilerParams(collective_id=0, has_side_effects=True, vmem_limit_bytes=VMEM),
        )(x, gain, wq, wk, wv, wo, jnp.asarray(table))

    tokens, whole = P(("dp", "sp"), None), P(None, None)
    return jax.shard_map(
        step,
        mesh=mesh,
        in_specs=(tokens, P(None), whole, whole, whole, whole),
        out_specs=tokens,
        check_vma=False,
    )
```
